32 devices in a mesh: batch: 4 (over y, x), centre: 8 (over z, core).
Axes of the slice: x: 2, y: 2, z: 4, core: 2. Of those that a mesh axis runs over, the one named last changes fastest.
Arguments:
- pool: float32 [1024, 1024], P('batch', 'centre'), may hold values from -4.5 to 4.5
- sample_index: int32 [512], P('batch'), may hold values from 0 to 255
- targets: float32 [512, 256], P('batch'), may hold values from -6 to 6
- centres: float32 [512, 1024], P(('batch', 'centre')), may hold values from -4.5 to 4.5
- coeffs: float32 [512, 256], P(('batch', 'centre')), may hold values from -6 to 6
- eigvecs: float32 [512, 1024], P(('batch', 'centre')), may hold values from -0.75 to 0.75
- eigscale: float32 [1024], replicated, may hold values from 0.1 to 0.95
Outputs:
- new_coeffs: float32 [512, 256], P(('batch', 'centre'))
The draws below stay inside these ranges and needn't reach their ends.
Inputs may be any that keep to these rules, and one draw needn't show every extreme that they name: `sample_index`: each batch row's sample lies in the block of 256 training samples held by its own batch group; the index counts within that block.
All inputs are finite; a program needn't handle non-finite values.
Results may differ from the reference program's by a relative error of at most 0.0003.
Values sent between devices are 32-bit elements; how exact they have to be, the bound alone decides.
A program may use at most 64 MiB of HBM per device.

```python
import jax
import jax.numpy as jnp
from jax import lax

FEATURES = 1024
OUTPUTS = 256
EIGEN = 1024
ROWS_DEV = 128
SAMPLES_DEV = 256
ROWS = 512
CENTRES = 512
POOL = 1024
N_BATCH = 4


def plant(array, rng, least, high):
    dims = array.shape
    place = [jax.random.randint(jax.random.fold_in(rng, axis), (), 0, dims[axis]) for axis in range(len(dims))]
    array = array.at[tuple(place)].set(least)
    longest = dims.index(max(dims))
    place[longest] = (place[longest] + 1) % dims[longest]
    return array.at[tuple(place)].set(high)


def block_scale(own_key, extent, cuts, low, top_value):
    level, own = 1.0, jax.random.fold_in(own_key, 6)
    for axis_at, shards_of in cuts:
        draws = jnp.exp(jax.random.uniform(jax.random.fold_in(own, axis_at), (shards_of,), jnp.float32, low / len(cuts), top_value / len(cuts)))
        level = level * jnp.repeat(draws, extent[axis_at] // shards_of).reshape([-1 if axis == axis_at else 1 for axis in range(len(extent))])
    return level


def bell_draw(own_key, dims, width, limit, shards=(), held_as=jnp.bfloat16):
    gain = block_scale(own_key, dims, shards, -0.22, 0.18) if shards else 1.0
    values = jax.random.normal(own_key, dims, jnp.float32) * width * gain
    return jnp.minimum(jnp.maximum(values, -limit), limit).astype(held_as)


def setup_inputs(seed: int = 0) -> dict:
    key_of = jax.random.split(jax.random.key(seed), 8)
    return {
        "pool": bell_draw(key_of[0], (POOL, FEATURES), 0.75, 4.5, ((0, 4), (1, 8)), jnp.float32),
        "sample_index": plant(jax.random.randint(key_of[1], (ROWS,), 0, SAMPLES_DEV), jax.random.fold_in(key_of[1], 1), 0, SAMPLES_DEV - 1).astype(jnp.int32),
        "targets": bell_draw(key_of[2], (ROWS, OUTPUTS), 1.0, 6.0, ((0, 4),), jnp.float32),
        "centres": bell_draw(key_of[3], (CENTRES, FEATURES), 0.75, 4.5, ((0, 32),), jnp.float32),
        "coeffs": bell_draw(key_of[4], (CENTRES, OUTPUTS), 1.0, 6.0, ((0, 32),), jnp.float32),
        "eigvecs": bell_draw(key_of[5], (CENTRES, EIGEN), (CENTRES // 8) ** -0.5, 0.75, ((0, 32),), jnp.float32),
        "eigscale": jnp.clip(jax.random.uniform(key_of[6], (EIGEN,), jnp.float32, 0.1, 0.95), 0.1, 0.95),
    }


def reference(pool, sample_index, targets, centres, coeffs, eigvecs, eigscale):
    highest = lax.Precision.HIGHEST
    owner = jnp.arange(ROWS, dtype=jnp.int32) // ROWS_DEV
    picks = (owner * SAMPLES_DEV + sample_index).astype(jnp.int32)
    batch_x = jnp.take(pool, picks, axis=0)
    inv_width = 1.0 / jnp.sqrt(jnp.float32(FEATURES))
    model_norm = 1.0 / jnp.sqrt(jnp.float32(CENTRES))
    blocks = N_BATCH
    block_rows = CENTRES // blocks
    zs = centres.reshape(blocks, block_rows, FEATURES)
    cs = coeffs.reshape(blocks, block_rows, OUTPUTS)

    def kernel_block(zblock):
        return jnp.exp(jnp.dot(batch_x, zblock.T, precision=highest, preferred_element_type=jnp.float32) * inv_width)

    def add_pred(totals, pieces):
        zblock, cblock = pieces
        return (totals + jnp.dot(kernel_block(zblock), cblock, precision=highest, preferred_element_type=jnp.float32), None)
    summed, unused = lax.scan(add_pred, jnp.zeros((ROWS, OUTPUTS), jnp.float32), (zs, cs))
    residual = summed * model_norm - targets

    def grad_block(zblock):
        return jnp.dot(kernel_block(zblock).T, residual, precision=highest, preferred_element_type=jnp.float32)
    gradient = lax.map(grad_block, zs).reshape(CENTRES, OUTPUTS) * model_norm
    coords = jnp.dot(eigvecs.T, gradient, precision=highest, preferred_element_type=jnp.float32)
    correction = jnp.dot(eigvecs, eigscale[:, None] * coords, precision=highest, preferred_element_type=jnp.float32)
    step_size = 0.5 * jnp.sqrt(jnp.float32(CENTRES) / jnp.float32(ROWS))
    return coeffs - step_size * (gradient - correction)
```

```python
import jax
import jax.numpy as jnp
from jax import lax
from jax.experimental import pallas as pl
from jax.experimental.pallas import tpu as pltpu
from jax.sharding import PartitionSpec as P

MESH = pl.DeviceIdType.MESH
F32 = jnp.float32


def mm(a, b, dims):
    return lax.dot_general(
        a, b, (dims, ((), ())), precision=lax.Precision.HIGHEST, preferred_element_type=F32
    )


NN = ((1,), (0,))
NT = ((1,), (1,))


def farthest_first(z, n):
    side = z // (n // 2)
    near = z + side * (n - 1 - 2 * z)
    lone = n - 1 - 2 * near
    order = []
    for k in range(n - 1):
        paired = (k - lone + n) // n
        step = paired * (k - lone)
        beyond = near + (1 - 2 * (step % 2)) * (near - step // 2)
        chip = (1 - paired) * (n - 1 - k) + paired * beyond
        order.append(chip + side * (n - 1 - 2 * chip))
    return order


def flipped(b, k):
    bit = 1
    while bit <= k:
        if k & bit:
            b = b + bit * (1 - 2 * ((b // bit) % 2))
        bit *= 2
    return b


def flat(value):
    count, depth, width = value.shape
    if depth % 8 == 0:
        return value.reshape(count * depth, width)
    return jnp.concatenate([value[j] for j in range(count)], axis=0)


def step_kernel(
    nb, nc, inv_width, model_norm, step_size,
    pool_hbm, i_hbm, t_hbm, z_hbm, a_hbm, e_hbm, s_hbm, out_ref,
    pool_ref, i_ref, t_ref, s_ref, local,
    xg, xs, zp, zcol, ep, ej, ca, ks, mo, mt, po, fin,
    x_send, x_recv, zp_send, zp_recv, ep_send, ep_recv, ej_send, ej_recv,
    cz_send, cz_recv, cp_send, cp_recv, k_send, k_recv, m_send, m_recv, f_send, f_recv,
):
    b = lax.axis_index("batch")
    c = lax.axis_index("centre")
    nz = nc // 2
    nq = 2 * nb
    z = c // 2
    core = lax.rem(c, 2)
    mate = c + 1 - 2 * core
    own = z_hbm.shape[0]
    width = pool_hbm.shape[1]
    half = t_hbm.shape[1]
    plane = nq * own
    q = 2 * b + core
    chips = farthest_first(z, nz)
    if nb & (nb - 1):
        groups = [lax.rem(b + k, nb) for k in range(1, nb)]
    else:
        groups = [flipped(b, k) for k in range(nb - 1, 0, -1)]
    pending = []

    def push(src, dst, send, recv, bi, ci):
        copy = pltpu.make_async_remote_copy(
            src_ref=src, dst_ref=dst, send_sem=send, recv_sem=recv,
            device_id=(bi, ci), device_id_type=MESH,
        )
        copy.start()
        pending.append(copy)

    def arrived(dst, recv):
        pltpu.make_async_remote_copy(
            src_ref=dst, dst_ref=dst, send_sem=recv, recv_sem=recv,
            device_id=(b, mate), device_id_type=MESH,
        ).wait_recv()

    barrier = pltpu.get_barrier_semaphore()
    for chip in chips:
        for side in (core, 1 - core):
            pl.semaphore_signal(barrier, inc=1, device_id=(b, 2 * chip + side), device_id_type=MESH)
    for bi in groups:
        for ci in (c, mate):
            pl.semaphore_signal(barrier, inc=1, device_id=(bi, ci), device_id_type=MESH)
    pl.semaphore_signal(barrier, inc=1, device_id=(b, mate), device_id_type=MESH)
    fetches = []
    for k, (src, dst) in enumerate([
        (pool_hbm, pool_ref), (i_hbm, i_ref), (z_hbm, zp.at[q]), (e_hbm, ep.at[q]),
        (e_hbm, ej.at[z]), (a_hbm, ca.at[z, q]), (s_hbm, s_ref), (t_hbm.at[core], t_ref),
    ]):
        copy = pltpu.make_async_copy(src, dst, local.at[k])
        copy.start()
        fetches.append(copy)
    fetches[0].wait()
    fetches[1].wait()
    rows = i_ref.shape[1]
    lines = lax.broadcasted_iota(jnp.int32, (pool_ref.shape[0], rows), 0)
    chosen = jnp.where(lines == i_ref[...], 1.0, 0.0).astype(F32)
    picked = mm(chosen, pool_ref[...], ((0,), (0,)))
    for h in range(2):
        xg[h] = picked[h * half:(h + 1) * half]
    xs[c] = xg[core]
    for copy in fetches[2:]:
        copy.wait()
    pl.semaphore_wait(barrier, nc - 1 + 2 * (nb - 1))

    for k, chip in enumerate(chips):
        for j, side in enumerate((core, 1 - core)):
            push(xg.at[side], xs.at[c], x_send.at[2 * k + j], x_recv.at[c], b, 2 * chip + side)
    push(xg.at[1 - core], xs.at[c], x_send.at[nc - 2], x_recv.at[c], b, mate)
    for k, bi in enumerate(groups):
        push(zp.at[q], zp.at[q], zp_send.at[k], zp_recv.at[q], bi, c)
    push(zp.at[q], zp.at[q], zp_send.at[nb - 1], zp_recv.at[q], b, mate)
    for k, bi in enumerate(groups):
        push(ep.at[q], ep.at[q], ep_send.at[k], ep_recv.at[q], bi, c)
    push(ep.at[q], ep.at[q], ep_send.at[nb - 1], ep_recv.at[q], b, mate)
    for k, chip in enumerate(chips):
        push(ca.at[z, q], ca.at[z, q], cz_send.at[k], cz_recv.at[z], b, 2 * chip + core)
    for k, chip in enumerate(chips):
        push(ej.at[z], ej.at[z], ej_send.at[k], ej_recv.at[z], b, 2 * chip + core)

    for k, bi in enumerate(groups):
        qi = 2 * bi + core
        arrived(zp.at[qi], zp_recv.at[qi])
        push(zp.at[qi], zp.at[qi], zp_send.at[nb + k], zp_recv.at[qi], b, mate)
    arrived(zp.at[2 * b + 1 - core], zp_recv.at[2 * b + 1 - core])
    for bi in groups:
        qi = 2 * bi + 1 - core
        arrived(zp.at[qi], zp_recv.at[qi])
    for j in range(nc):
        zcol[j] = flat(zp[:, :, j * width:(j + 1) * width])
    for k, bi in enumerate(groups):
        qi = 2 * bi + core
        arrived(ep.at[qi], ep_recv.at[qi])
        push(ep.at[qi], ep.at[qi], ep_send.at[nb + k], ep_recv.at[qi], b, mate)

    scores = mm(xs[c], zcol[c], NT)
    arrived(xs.at[mate], x_recv.at[mate])
    scores = scores + mm(xs[mate], zcol[mate], NT)
    for chip in chips:
        for side in (core, 1 - core):
            ci = 2 * chip + side
            arrived(xs.at[ci], x_recv.at[ci])
            scores = scores + mm(xs[ci], zcol[ci], NT)
    kernel = jnp.exp(scores * inv_width)
    ks[z] = kernel
    for k, chip in enumerate(chips):
        push(ks.at[z], ks.at[z], k_send.at[k], k_recv.at[z], b, 2 * chip + core)

    for chip in chips:
        arrived(ca.at[chip, q], cz_recv.at[chip])
    for k, bi in enumerate(groups):
        push(ca.at[:, q], ca.at[:, q], cp_send.at[k], cp_recv.at[q], bi, c)
    push(ca.at[:, q], ca.at[:, q], cp_send.at[nb - 1], cp_recv.at[q], b, mate)

    arrived(ep.at[2 * b + 1 - core], ep_recv.at[2 * b + 1 - core])
    for bi in groups:
        qi = 2 * bi + 1 - core
        arrived(ep.at[qi], ep_recv.at[qi])
    planes = flat(ep[...])
    scale = s_ref[...]
    mo[z] = mm(ej[z] * scale, planes, NT)
    for chip in chips:
        arrived(ej.at[chip], ej_recv.at[chip])
        mo[chip] = mm(ej[chip] * scale, planes, NT)
    for k, bi in enumerate(groups):
        for j, ci in enumerate((c, mate)):
            push(mo, mt.at[:, q], m_send.at[2 * k + j], m_recv.at[q], bi, ci)
    push(mo, mt.at[:, q], m_send.at[2 * nb - 2], m_recv.at[q], b, mate)
    mt[:, q] = mo[...]

    for k, bi in enumerate(groups):
        qi = 2 * bi + core
        arrived(ca.at[:, qi], cp_recv.at[qi])
        push(ca.at[:, qi], ca.at[:, qi], cp_send.at[nb + k], cp_recv.at[qi], b, mate)
    arrived(ca.at[:, 2 * b + 1 - core], cp_recv.at[2 * b + 1 - core])
    for bi in groups:
        qi = 2 * bi + 1 - core
        arrived(ca.at[:, qi], cp_recv.at[qi])

    value = mm(kernel, flat(ca[z]), NN)
    for chip in chips:
        arrived(ks.at[chip], k_recv.at[chip])
        value = value + mm(ks[chip], flat(ca[chip]), NN)
    residual = value * model_norm - t_ref[...]

    arrived(mt.at[:, 2 * b + 1 - core], m_recv.at[2 * b + 1 - core])
    for bi in groups:
        for side in (core, 1 - core):
            qi = 2 * bi + side
            arrived(mt.at[:, qi], m_recv.at[qi])
    weights = kernel
    for j in range(nz):
        weights = weights - mm(ks[j], flat(mt[j]), NN)
    partial = mm(weights.T, residual, NN)
    for j in range(nq):
        po[j] = partial[j * own:(j + 1) * own]
    for k, bi in enumerate(groups):
        for j, side in enumerate((core, 1 - core)):
            push(po.at[2 * bi + side], fin.at[q], f_send.at[2 * k + j], f_recv.at[q], bi, 2 * z + side)
    push(po.at[2 * b + 1 - core], fin.at[q], f_send.at[2 * nb - 2], f_recv.at[q], b, mate)
    total = po[q]
    arrived(fin.at[2 * b + 1 - core], f_recv.at[2 * b + 1 - core])
    total = total + fin[2 * b + 1 - core]
    for bi in groups:
        for side in (core, 1 - core):
            qi = 2 * bi + side
            arrived(fin.at[qi], f_recv.at[qi])
            total = total + fin[qi]
    out_ref[...] = ca[z, q] - (step_size * model_norm) * total
    for copy in pending:
        copy.wait_send()


def on_device(pool, sample_index, targets, centres, coeffs, eigvecs, eigscale):
    nb = lax.axis_size("batch")
    nc = lax.axis_size("centre")
    nz = nc // 2
    nq = 2 * nb
    rows = sample_index.shape[0]
    half = rows // 2
    width = pool.shape[1]
    own, features = centres.shape
    outputs = targets.shape[1]
    eigen = eigvecs.shape[1]
    plane = own * nq
    total_centres = own * nb * nc
    body = lambda *refs: step_kernel(
        nb, nc, features ** -0.5, total_centres ** -0.5,
        0.5 * (total_centres / (rows * nb)) ** 0.5, *refs
    )
    dma = pltpu.SemaphoreType.DMA
    vmem = lambda *dims: pltpu.VMEM(dims, F32)
    return pl.pallas_call(
        body,
        out_shape=jax.ShapeDtypeStruct((own, outputs), F32),
        in_specs=[pl.BlockSpec(memory_space=pltpu.HBM)] * 7,
        out_specs=pl.BlockSpec(memory_space=pltpu.VMEM),
        scratch_shapes=[
            vmem(*pool.shape),
            pltpu.VMEM((1, rows), jnp.int32),
            vmem(half, outputs),
            vmem(1, eigen),
            dma((8,)),
            vmem(2, half, width),
            vmem(nc, half, width),
            vmem(nq, own, features),
            vmem(nc, plane, width),
            vmem(nq, own, eigen),
            vmem(nz, own, eigen),
            vmem(nz, nq, own, outputs),
            vmem(nz, half, plane),
            vmem(nz, own, plane),
            vmem(nz, nq, own, plane),
            vmem(nq, own, outputs),
            vmem(nq, own, outputs),
            dma((nc,)), dma((nc,)),
            dma((nq,)), dma((nq,)),
            dma((nq,)), dma((nq,)),
            dma((nz,)), dma((nz,)),
            dma((nz,)), dma((nz,)),
            dma((nq,)), dma((nq,)),
            dma((nz,)), dma((nz,)),
            dma((nq,)), dma((nq,)),
            dma((nq,)), dma((nq,)),
        ],
        compiler_params=pltpu.CompilerParams(
            collective_id=0, has_side_effects=True, vmem_limit_bytes=67043328
        ),
    )(
        pool,
        sample_index[None, :],
        targets.reshape(2, half, outputs),
        centres,
        coeffs,
        eigvecs,
        eigscale[None, :],
    )


def solution(mesh):
    return jax.shard_map(
        on_device,
        mesh=mesh,
        in_specs=(
            P("batch", "centre"),
            P("batch"),
            P("batch", None),
            P(("batch", "centre"), None),
            P(("batch", "centre"), None),
            P(("batch", "centre"), None),
            P(),
        ),
        out_specs=P(("batch", "centre"), None),
        check_vma=False,
    )
```

```python
import jax
import jax.numpy as jnp
from jax import lax
from jax.experimental import pallas as pl
from jax.experimental.pallas import tpu as pltpu
from jax.sharding import PartitionSpec as P

MESH = pl.DeviceIdType.MESH
F32 = jnp.float32
BF16 = jnp.bfloat16


def mm(a, b, dims):
    return lax.dot_general(
        a, b, (dims, ((), ())), precision=lax.Precision.HIGHEST, preferred_element_type=F32
    )


def split(value):
    high = value.astype(BF16)
    return high, (value - high.astype(F32)).astype(BF16)


def mm3(a, b, dims):
    def one(left, right):
        return lax.dot_general(left, right, (dims, ((), ())), preferred_element_type=F32)

    return one(a[0], b[0]) + (one(a[0], b[1]) + one(a[1], b[0]))


NN = ((1,), (0,))
NT = ((1,), (1,))


def farthest_first(z, n):
    side = z // (n // 2)
    near = z + side * (n - 1 - 2 * z)
    lone = n - 1 - 2 * near
    order = []
    for k in range(n - 1):
        paired = (k - lone + n) // n
        step = paired * (k - lone)
        beyond = near + (1 - 2 * (step % 2)) * (near - step // 2)
        chip = (1 - paired) * (n - 1 - k) + paired * beyond
        order.append(chip + side * (n - 1 - 2 * chip))
    return order


def flipped(b, k):
    bit = 1
    while bit <= k:
        if k & bit:
            b = b + bit * (1 - 2 * ((b // bit) % 2))
        bit *= 2
    return b


def flat(value):
    count, depth, width = value.shape
    if depth % 8 == 0:
        return value.reshape(count * depth, width)
    return jnp.concatenate([value[j] for j in range(count)], axis=0)


def step_kernel(
    nb, nc, inv_width, model_norm, step_size,
    pool_hbm, i_hbm, t_hbm, z_hbm, a_hbm, e_hbm, s_hbm, out_ref,
    pool_ref, i_ref, t_ref, s_ref, local,
    xg, xs, zp, zh, zl, ep, ej, ca, ks, mo, mt, po, fin,
    x_send, x_recv, zp_send, zp_recv, ep_send, ep_recv, ej_send, ej_recv,
    cz_send, cz_recv, cp_send, cp_recv, k_send, k_recv, m_send, m_recv, f_send, f_recv,
):
    b = lax.axis_index("batch")
    c = lax.axis_index("centre")
    nz = nc // 2
    nq = 2 * nb
    z = c // 2
    core = lax.rem(c, 2)
    mate = c + 1 - 2 * core
    own = z_hbm.shape[0]
    width = pool_hbm.shape[1]
    half = t_hbm.shape[1]
    plane = nq * own
    q = 2 * b + core
    chips = farthest_first(z, nz)
    if nb & (nb - 1):
        groups = [lax.rem(b + k, nb) for k in range(1, nb)]
    else:
        groups = [flipped(b, k) for k in range(nb - 1, 0, -1)]
    pending = []

    def push(src, dst, send, recv, bi, ci):
        copy = pltpu.make_async_remote_copy(
            src_ref=src, dst_ref=dst, send_sem=send, recv_sem=recv,
            device_id=(bi, ci), device_id_type=MESH,
        )
        copy.start()
        pending.append(copy)

    def arrived(dst, recv):
        pltpu.make_async_remote_copy(
            src_ref=dst, dst_ref=dst, send_sem=recv, recv_sem=recv,
            device_id=(b, mate), device_id_type=MESH,
        ).wait_recv()

    barrier = pltpu.get_barrier_semaphore()
    for chip in chips:
        for side in (core, 1 - core):
            pl.semaphore_signal(barrier, inc=1, device_id=(b, 2 * chip + side), device_id_type=MESH)
    for bi in groups:
        for ci in (c, mate):
            pl.semaphore_signal(barrier, inc=1, device_id=(bi, ci), device_id_type=MESH)
    pl.semaphore_signal(barrier, inc=1, device_id=(b, mate), device_id_type=MESH)
    fetches = []
    for k, (src, dst) in enumerate([
        (pool_hbm, pool_ref), (i_hbm, i_ref), (z_hbm, zp.at[q]), (e_hbm, ep.at[q]),
        (e_hbm, ej.at[z]), (a_hbm, ca.at[z, q]), (s_hbm, s_ref), (t_hbm.at[core], t_ref),
    ]):
        copy = pltpu.make_async_copy(src, dst, local.at[k])
        copy.start()
        fetches.append(copy)
    fetches[0].wait()
    fetches[1].wait()
    rows = i_ref.shape[1]
    lines = lax.broadcasted_iota(jnp.int32, (pool_ref.shape[0], rows), 0)
    chosen = jnp.where(lines == i_ref[...], 1.0, 0.0).astype(F32)
    picked = mm(chosen, pool_ref[...], ((0,), (0,)))
    for h in range(2):
        xg[h] = picked[h * half:(h + 1) * half]
    xs[c] = xg[core]
    for copy in fetches[2:]:
        copy.wait()
    pl.semaphore_wait(barrier, nc - 1 + 2 * (nb - 1))

    for k, chip in enumerate(chips):
        push(ca.at[z, q], ca.at[z, q], cz_send.at[k], cz_recv.at[z], b, 2 * chip + core)
    for k, chip in list(enumerate(chips))[:1]:
        push(ej.at[z], ej.at[z], ej_send.at[k], ej_recv.at[z], b, 2 * chip + core)
    for k, chip in enumerate(chips):
        for j, side in enumerate((core, 1 - core)):
            push(xg.at[side], xs.at[c], x_send.at[2 * k + j], x_recv.at[c], b, 2 * chip + side)
    push(xg.at[1 - core], xs.at[c], x_send.at[nc - 2], x_recv.at[c], b, mate)
    for k, chip in list(enumerate(chips))[1:]:
        push(ej.at[z], ej.at[z], ej_send.at[k], ej_recv.at[z], b, 2 * chip + core)
    for k, bi in enumerate(groups):
        push(zp.at[q], zp.at[q], zp_send.at[k], zp_recv.at[q], bi, c)
    push(zp.at[q], zp.at[q], zp_send.at[nb - 1], zp_recv.at[q], b, mate)
    for k, bi in enumerate(groups):
        push(ep.at[q], ep.at[q], ep_send.at[k], ep_recv.at[q], bi, c)
    push(ep.at[q], ep.at[q], ep_send.at[nb - 1], ep_recv.at[q], b, mate)

    twin = 2 * b + 1 - core
    near = [2 * bi + core for bi in groups]
    cross = [2 * bi + 1 - core for bi in groups]
    for chip in chips:
        arrived(ca.at[chip, q], cz_recv.at[chip])
    for k, bi in enumerate(groups):
        push(ca.at[:, q], ca.at[:, q], cp_send.at[k], cp_recv.at[q], bi, c)
    push(ca.at[:, q], ca.at[:, q], cp_send.at[nb - 1], cp_recv.at[q], b, mate)
    for k, qi in enumerate(near):
        arrived(zp.at[qi], zp_recv.at[qi])
        push(zp.at[qi], zp.at[qi], zp_send.at[nb + k], zp_recv.at[qi], b, mate)
    for qi in [twin] + cross:
        arrived(zp.at[qi], zp_recv.at[qi])
    for j in range(nc):
        zh[j], zl[j] = split(flat(zp[:, :, j * width:(j + 1) * width]))

    def score(ci):
        return mm3(split(xs[ci]), (zh[ci], zl[ci]), NT)

    scores = score(c)
    arrived(xs.at[mate], x_recv.at[mate])
    scores = scores + score(mate)
    for k, qi in enumerate(near):
        arrived(ep.at[qi], ep_recv.at[qi])
        push(ep.at[qi], ep.at[qi], ep_send.at[nb + k], ep_recv.at[qi], b, mate)
    for chip in chips:
        for side in (core, 1 - core):
            ci = 2 * chip + side
            arrived(xs.at[ci], x_recv.at[ci])
            scores = scores + score(ci)
    kernel = jnp.exp(scores * inv_width)
    ks[z] = kernel
    for k, chip in enumerate(chips):
        push(ks.at[z], ks.at[z], k_send.at[k], k_recv.at[z], b, 2 * chip + core)

    for k, qi in enumerate(near):
        arrived(ca.at[:, qi], cp_recv.at[qi])
        push(ca.at[:, qi], ca.at[:, qi], cp_send.at[nb + k], cp_recv.at[qi], b, mate)
    for qi in [twin] + cross:
        arrived(ep.at[qi], ep_recv.at[qi])
    planes = split(flat(ep[...]) * s_ref[...])
    for n, chip in enumerate([z] + chips):
        if n:
            arrived(ej.at[chip], ej_recv.at[chip])
        block = mm3(split(ej[chip]), planes, NT)
        mo[chip] = block
        for k, bi in enumerate(groups):
            for j, ci in enumerate((c, mate)):
                push(mo.at[chip], mt.at[chip, q], m_send.at[n, 2 * k + j], m_recv.at[chip, q], bi, ci)
        push(mo.at[chip], mt.at[chip, q], m_send.at[n, 2 * nb - 2], m_recv.at[chip, q], b, mate)
        mt[chip, q] = block

    for qi in [twin] + cross:
        arrived(ca.at[:, qi], cp_recv.at[qi])
    weighed = [split(kernel)]
    value = mm3(weighed[0], split(flat(ca[z])), NN)
    for chip in chips:
        coeffs = split(flat(ca[chip]))
        arrived(ks.at[chip], k_recv.at[chip])
        weighed.append(split(ks[chip]))
        value = value + mm3(weighed[-1], coeffs, NN)
    residual = split(value * model_norm - t_ref[...])

    weights = kernel
    for n, chip in enumerate([z] + chips):
        for qi in [twin] + near + cross:
            arrived(mt.at[chip, qi], m_recv.at[chip, qi])
        weights = weights - mm3(weighed[n], split(flat(mt[chip])), NN)
    partial = mm3(split(weights.T), residual, NN)
    for j in range(nq):
        po[j] = partial[j * own:(j + 1) * own]
    for k, bi in enumerate(groups):
        for j, side in enumerate((core, 1 - core)):
            push(po.at[2 * bi + side], fin.at[q], f_send.at[2 * k + j], f_recv.at[q], bi, 2 * z + side)
    push(po.at[twin], fin.at[q], f_send.at[2 * nb - 2], f_recv.at[q], b, mate)
    total = po[q]
    for qi in [twin] + near + cross:
        arrived(fin.at[qi], f_recv.at[qi])
        total = total + fin[qi]
    out_ref[...] = ca[z, q] - (step_size * model_norm) * total
    for copy in pending:
        copy.wait_send()


def on_device(pool, sample_index, targets, centres, coeffs, eigvecs, eigscale):
    nb = lax.axis_size("batch")
    nc = lax.axis_size("centre")
    nz = nc // 2
    nq = 2 * nb
    rows = sample_index.shape[0]
    half = rows // 2
    width = pool.shape[1]
    own, features = centres.shape
    outputs = targets.shape[1]
    eigen = eigvecs.shape[1]
    plane = own * nq
    total_centres = own * nb * nc
    body = lambda *refs: step_kernel(
        nb, nc, features ** -0.5, total_centres ** -0.5,
        0.5 * (total_centres / (rows * nb)) ** 0.5, *refs
    )
    dma = pltpu.SemaphoreType.DMA
    vmem = lambda *dims: pltpu.VMEM(dims, F32)
    scratch = [
        vmem(*pool.shape),
        pltpu.VMEM((1, rows), jnp.int32),
        vmem(half, outputs),
        vmem(1, eigen),
        dma((8,)),
        vmem(2, half, width),
        vmem(nc, half, width),
        vmem(nq, own, features),
        pltpu.VMEM((nc, plane, width), BF16),
        pltpu.VMEM((nc, plane, width), BF16),
        vmem(nq, own, eigen),
        vmem(nz, own, eigen),
        vmem(nz, nq, own, outputs),
        vmem(nz, half, plane),
        vmem(nz, own, plane),
        vmem(nz, nq, own, plane),
        vmem(nq, own, outputs),
        vmem(nq, own, outputs),
        dma((nc,)), dma((nc,)),
        dma((nq,)), dma((nq,)),
        dma((nq,)), dma((nq,)),
        dma((nz,)), dma((nz,)),
        dma((nz,)), dma((nz,)),
        dma((nq,)), dma((nq,)),
        dma((nz,)), dma((nz,)),
        dma((nz, nq)), dma((nz, nq)),
        dma((nq,)), dma((nq,)),
    ]
    taken = 0
    for buffer in scratch:
        if buffer.memory_space == pltpu.VMEM:
            *outer, deep, wide = buffer.shape
            size = -(-deep // 8) * 8 * (-(-wide // 128) * 128) * 4
            for extent in outer:
                size *= extent
            taken += size
    return pl.pallas_call(
        body,
        out_shape=jax.ShapeDtypeStruct((own, outputs), F32),
        in_specs=[pl.BlockSpec(memory_space=pltpu.HBM)] * 7,
        out_specs=pl.BlockSpec(memory_space=pltpu.VMEM),
        scratch_shapes=scratch,
        compiler_params=pltpu.CompilerParams(
            collective_id=0, has_side_effects=True, vmem_limit_bytes=min(taken + (12 << 20), 67043328)
        ),
    )(*[
        pltpu.with_memory_space_constraint(operand, pltpu.HBM)
        for operand in (
            pool,
            sample_index[None, :],
            targets.reshape(2, half, outputs),
            centres,
            coeffs,
            eigvecs,
            eigscale[None, :],
        )
    ])


def solution(mesh):
    return jax.shard_map(
        on_device,
        mesh=mesh,
        in_specs=(
            P("batch", "centre"),
            P("batch"),
            P("batch", None),
            P(("batch", "centre"), None),
            P(("batch", "centre"), None),
            P(("batch", "centre"), None),
            P(),
        ),
        out_specs=P(("batch", "centre"), None),
        check_vma=False,
    )
```

```python
import jax
import jax.numpy as jnp
from jax import lax
from jax.experimental import pallas as pl
from jax.experimental.pallas import tpu as pltpu
from jax.sharding import PartitionSpec as P

MESH = pl.DeviceIdType.MESH
F32 = jnp.float32
BF16 = jnp.bfloat16


def mm(a, b, dims):
    return lax.dot_general(
        a, b, (dims, ((), ())), precision=lax.Precision.HIGHEST, preferred_element_type=F32
    )


def split(value):
    high = value.astype(BF16)
    return high, (value - high.astype(F32)).astype(BF16)


def mm3(a, b, dims):
    def one(left, right):
        return lax.dot_general(left, right, (dims, ((), ())), preferred_element_type=F32)

    rows = a[0].shape[0]
    both = one(jnp.concatenate(a, axis=0), b[0])
    return both[:rows] + (both[rows:] + one(a[0], b[1]))


NN = ((1,), (0,))
NT = ((1,), (1,))


def farthest_first(z, n):
    side = z // (n // 2)
    near = z + side * (n - 1 - 2 * z)
    lone = n - 1 - 2 * near
    order = []
    for k in range(n - 1):
        paired = (k - lone + n) // n
        step = paired * (k - lone)
        beyond = near + (1 - 2 * (step % 2)) * (near - step // 2)
        chip = (1 - paired) * (n - 1 - k) + paired * beyond
        order.append(chip + side * (n - 1 - 2 * chip))
    return order


def flipped(b, k):
    bit = 1
    while bit <= k:
        if k & bit:
            b = b + bit * (1 - 2 * ((b // bit) % 2))
        bit *= 2
    return b


def flat(value):
    count, depth, width = value.shape
    if depth % 8 == 0:
        return value.reshape(count * depth, width)
    return jnp.concatenate([value[j] for j in range(count)], axis=0)


def step_kernel(
    nb, nc, inv_width, model_norm, step_size,
    pool_hbm, i_hbm, t_hbm, z_hbm, a_hbm, e_hbm, s_hbm, out_ref,
    pool_ref, i_ref, t_ref, s_ref, local,
    xg, xs, zp, zh, zl, ep, eq, ej, ca, ks, me, mo, mt, po, fin,
    x_send, x_recv, zp_send, zp_recv, ep_send, ep_recv, eq_send, eq_recv, ej_send, ej_recv,
    cz_send, cz_recv, cp_send, cp_recv, k_send, k_recv, m_send, m_recv, f_send, f_recv,
):
    b = lax.axis_index("batch")
    c = lax.axis_index("centre")
    nz = nc // 2
    nq = 2 * nb
    z = c // 2
    core = lax.rem(c, 2)
    mate = c + 1 - 2 * core
    own = z_hbm.shape[0]
    width = pool_hbm.shape[1]
    half = t_hbm.shape[1]
    plane = nq * own
    q = 2 * b + core
    chips = farthest_first(z, nz)
    rank, parity = z // 2, lax.rem(z, 2)
    sib = z + 1 - 2 * parity
    kin = farthest_first(rank, nz // 2)
    if nb & (nb - 1):
        groups = [lax.rem(b + k, nb) for k in range(1, nb)]
    else:
        groups = [flipped(b, k) for k in range(nb - 1, 0, -1)]
    pending = []

    def push(src, dst, send, recv, bi, ci):
        copy = pltpu.make_async_remote_copy(
            src_ref=src, dst_ref=dst, send_sem=send, recv_sem=recv,
            device_id=(bi, ci), device_id_type=MESH,
        )
        copy.start()
        pending.append(copy)

    def arrived(dst, recv):
        pltpu.make_async_remote_copy(
            src_ref=dst, dst_ref=dst, send_sem=recv, recv_sem=recv,
            device_id=(b, mate), device_id_type=MESH,
        ).wait_recv()

    barrier = pltpu.get_barrier_semaphore()
    for chip in chips:
        for side in (core, 1 - core):
            pl.semaphore_signal(barrier, inc=1, device_id=(b, 2 * chip + side), device_id_type=MESH)
    for bi in groups:
        for ci in (c, mate, 2 * sib, 2 * sib + 1):
            pl.semaphore_signal(barrier, inc=1, device_id=(bi, ci), device_id_type=MESH)
    pl.semaphore_signal(barrier, inc=1, device_id=(b, mate), device_id_type=MESH)
    fetches = []
    for k, (src, dst) in enumerate([
        (pool_hbm, pool_ref), (i_hbm, i_ref), (z_hbm, zp.at[q]), (e_hbm, ep.at[q]),
        (a_hbm, ca.at[z, q]), (s_hbm, s_ref), (t_hbm.at[core], t_ref),
    ]):
        copy = pltpu.make_async_copy(src, dst, local.at[k])
        copy.start()
        fetches.append(copy)
    fetches[0].wait()
    fetches[1].wait()
    rows = i_ref.shape[1]
    lines = lax.broadcasted_iota(jnp.int32, (pool_ref.shape[0], rows), 0)
    chosen = jnp.where(lines == i_ref[...], 1.0, 0.0).astype(F32)
    picked = mm(chosen, pool_ref[...], ((0,), (0,)))
    for h in range(2):
        xg[h] = picked[h * half:(h + 1) * half]
    xs[c] = xg[core]
    for copy in fetches[2:]:
        copy.wait()
    pl.semaphore_wait(barrier, nc - 1 + 4 * (nb - 1))

    for k, chip in enumerate(chips):
        push(ca.at[z, q], ca.at[z, q], cz_send.at[k], cz_recv.at[z], b, 2 * chip + core)
    push(ep.at[q], eq.at[q], eq_send.at[nq], eq_recv.at[q], b, 2 * sib + core)
    for k, chip in enumerate(chips):
        for j, side in enumerate((core, 1 - core)):
            push(xg.at[side], xs.at[c], x_send.at[2 * k + j], x_recv.at[c], b, 2 * chip + side)
    push(xg.at[1 - core], xs.at[c], x_send.at[nc - 2], x_recv.at[c], b, mate)
    for k, other in enumerate(kin):
        push(ep.at[q], ej.at[rank], ej_send.at[k], ej_recv.at[rank], b, 2 * (2 * other + parity) + core)
    for k, bi in enumerate(groups):
        push(zp.at[q], zp.at[q], zp_send.at[k], zp_recv.at[q], bi, c)
    push(zp.at[q], zp.at[q], zp_send.at[nb - 1], zp_recv.at[q], b, mate)
    for k, bi in enumerate(groups):
        push(ep.at[q], ep.at[q], ep_send.at[k], ep_recv.at[q], bi, c)
    push(ep.at[q], ep.at[q], ep_send.at[nb - 1], ep_recv.at[q], b, mate)

    twin = 2 * b + 1 - core
    near = [2 * bi + core for bi in groups]
    cross = [2 * bi + 1 - core for bi in groups]
    arrived(eq.at[q], eq_recv.at[q])
    for k, bi in enumerate(groups):
        push(eq.at[q], eq.at[q], eq_send.at[k], eq_recv.at[q], bi, c)
    push(eq.at[q], eq.at[q], eq_send.at[nb - 1], eq_recv.at[q], b, mate)
    for chip in chips:
        arrived(ca.at[chip, q], cz_recv.at[chip])
    for k, bi in enumerate(groups):
        push(ca.at[:, q], ca.at[:, q], cp_send.at[k], cp_recv.at[q], bi, c)
    push(ca.at[:, q], ca.at[:, q], cp_send.at[nb - 1], cp_recv.at[q], b, mate)
    for k, qi in enumerate(near):
        arrived(zp.at[qi], zp_recv.at[qi])
        push(zp.at[qi], zp.at[qi], zp_send.at[nb + k], zp_recv.at[qi], b, mate)
    for qi in [twin] + cross:
        arrived(zp.at[qi], zp_recv.at[qi])
    for j in range(nc):
        zh[j], zl[j] = split(flat(zp[:, :, j * width:(j + 1) * width]))

    def score(ci):
        return mm3(split(xs[ci]), (zh[ci], zl[ci]), NT)

    scores = score(c)
    arrived(xs.at[mate], x_recv.at[mate])
    scores = scores + score(mate)
    for k, qi in enumerate(near):
        arrived(ep.at[qi], ep_recv.at[qi])
        push(ep.at[qi], ep.at[qi], ep_send.at[nb + k], ep_recv.at[qi], b, mate)
    for chip in chips:
        for side in (core, 1 - core):
            ci = 2 * chip + side
            arrived(xs.at[ci], x_recv.at[ci])
            scores = scores + score(ci)
    kernel = jnp.exp(scores * inv_width)
    ks[z] = kernel
    for k, chip in enumerate(chips):
        push(ks.at[z], ks.at[z], k_send.at[k], k_recv.at[z], b, 2 * chip + core)

    for qi in [twin] + cross:
        arrived(ep.at[qi], ep_recv.at[qi])
    planes = split(flat(ep[...]) * s_ref[...])
    me[parity] = mm3(split(ep[q]), planes, NT)
    me[1 - parity] = mm3(split(eq[q]), planes, NT)
    for k, bi in enumerate(groups):
        for j, ci in enumerate((c, mate)):
            push(me, mt.at[rank, :, q], m_send.at[0, 2 * k + j], m_recv.at[rank, parity, q], bi, ci)
    push(me, mt.at[rank, :, q], m_send.at[0, nq - 2], m_recv.at[rank, parity, q], b, mate)
    mt[rank, :, q] = me[...]
    for k, qi in enumerate(near):
        arrived(eq.at[qi], eq_recv.at[qi])
        push(eq.at[qi], eq.at[qi], eq_send.at[nb + k], eq_recv.at[qi], b, mate)
    for n, other in enumerate(kin):
        arrived(ej.at[other], ej_recv.at[other])
        lines = split(ej[other])
        here = mt.at[other, parity, q]
        mo[n, 0] = mm3(lines, planes, NT)
        for k, bi in enumerate(groups):
            for j, ci in enumerate((c, mate)):
                push(mo.at[n, 0], here, m_send.at[n + 1, 2 * k + j], m_recv.at[other, parity, q], bi, ci)
        push(mo.at[n, 0], here, m_send.at[n + 1, nq - 2], m_recv.at[other, parity, q], b, mate)
        mt[other, parity, q] = mo[n, 0]
    for qi in [twin] + cross:
        arrived(eq.at[qi], eq_recv.at[qi])
    sibs = split(flat(eq[...]) * s_ref[...])
    for n, other in enumerate(kin):
        lines = split(ej[other])
        here = mt.at[other, parity, q]
        mo[n, 1] = mm3(lines, sibs, NT)
        for k, bi in enumerate(groups):
            for side in range(2):
                push(mo.at[n, 1], here, m_send.at[n + 1, nq + 2 * k + side], m_recv.at[other, parity, q], bi, 2 * sib + side)
        for side in range(2):
            push(mo.at[n, 1], here, m_send.at[n + 1, 2 * nq - 2 + side], m_recv.at[other, parity, q], b, 2 * sib + side)

    for k, qi in enumerate(near):
        arrived(ca.at[:, qi], cp_recv.at[qi])
        push(ca.at[:, qi], ca.at[:, qi], cp_send.at[nb + k], cp_recv.at[qi], b, mate)
    for qi in [twin] + cross:
        arrived(ca.at[:, qi], cp_recv.at[qi])
    value = mm3(split(kernel), split(flat(ca[z])), NN)
    for chip in chips:
        coeffs = split(flat(ca[chip]))
        arrived(ks.at[chip], k_recv.at[chip])
        value = value + mm3(split(ks[chip]), coeffs, NN)
    residual = split(value * model_norm - t_ref[...])

    weights = kernel
    for qi in [twin] + near + cross:
        arrived(mt.at[rank, :, qi], m_recv.at[rank, parity, qi])
    for n, other in enumerate([rank] + kin):
        if n:
            for qi in [twin] + near + cross:
                arrived(mt.at[other, parity, qi], m_recv.at[other, parity, qi])
            for qi in [q, twin] + near + cross:
                arrived(mt.at[other, 1 - parity, qi], m_recv.at[other, 1 - parity, qi])
        for side in range(2):
            weights = weights - mm3(split(ks[2 * other + side]), split(flat(mt[other, side])), NN)
    partial = mm3(split(weights.T), residual, NN)
    for j in range(nq):
        po[j] = partial[j * own:(j + 1) * own]
    for k, bi in enumerate(groups):
        for j, side in enumerate((core, 1 - core)):
            push(po.at[2 * bi + side], fin.at[q], f_send.at[2 * k + j], f_recv.at[q], bi, 2 * z + side)
    push(po.at[twin], fin.at[q], f_send.at[2 * nb - 2], f_recv.at[q], b, mate)
    total = po[q]
    for qi in [twin] + near + cross:
        arrived(fin.at[qi], f_recv.at[qi])
        total = total + fin[qi]
    out_ref[...] = ca[z, q] - (step_size * model_norm) * total
    for copy in pending:
        copy.wait_send()


def on_device(pool, sample_index, targets, centres, coeffs, eigvecs, eigscale):
    nb = lax.axis_size("batch")
    nc = lax.axis_size("centre")
    nz = nc // 2
    nq = 2 * nb
    rows = sample_index.shape[0]
    half = rows // 2
    width = pool.shape[1]
    own, features = centres.shape
    outputs = targets.shape[1]
    eigen = eigvecs.shape[1]
    plane = own * nq
    total_centres = own * nb * nc
    body = lambda *refs: step_kernel(
        nb, nc, features ** -0.5, total_centres ** -0.5,
        0.5 * (total_centres / (rows * nb)) ** 0.5, *refs
    )
    dma = pltpu.SemaphoreType.DMA
    vmem = lambda *dims: pltpu.VMEM(dims, F32)
    scratch = [
        vmem(*pool.shape),
        pltpu.VMEM((1, rows), jnp.int32),
        vmem(half, outputs),
        vmem(1, eigen),
        dma((8,)),
        vmem(2, half, width),
        vmem(nc, half, width),
        vmem(nq, own, features),
        pltpu.VMEM((nc, plane, width), BF16),
        pltpu.VMEM((nc, plane, width), BF16),
        vmem(nq, own, eigen),
        vmem(nq, own, eigen),
        vmem(nz // 2, own, eigen),
        vmem(nz, nq, own, outputs),
        vmem(nz, half, plane),
        vmem(2, own, plane),
        vmem(nz // 2 - 1, 2, own, plane),
        vmem(nz // 2, 2, nq, own, plane),
        vmem(nq, own, outputs),
        vmem(nq, own, outputs),
        dma((nc,)), dma((nc,)),
        dma((nq,)), dma((nq,)),
        dma((nq,)), dma((nq,)),
        dma((nq + 1,)), dma((nq,)),
        dma((nz,)), dma((nz,)),
        dma((nz,)), dma((nz,)),
        dma((nq,)), dma((nq,)),
        dma((nz,)), dma((nz,)),
        dma((nz // 2, 2 * nq)), dma((nz // 2, 2, nq)),
        dma((nq,)), dma((nq,)),
    ]
    taken = 0
    for buffer in scratch:
        if buffer.memory_space == pltpu.VMEM:
            *outer, deep, wide = buffer.shape
            size = -(-deep // 8) * 8 * (-(-wide // 128) * 128) * 4
            for extent in outer:
                size *= extent
            taken += size
    return pl.pallas_call(
        body,
        out_shape=jax.ShapeDtypeStruct((own, outputs), F32),
        in_specs=[pl.BlockSpec(memory_space=pltpu.HBM)] * 7,
        out_specs=pl.BlockSpec(memory_space=pltpu.VMEM),
        scratch_shapes=scratch,
        compiler_params=pltpu.CompilerParams(
            collective_id=0, has_side_effects=True, vmem_limit_bytes=min(taken + (12 << 20), 67043328)
        ),
    )(*[
        pltpu.with_memory_space_constraint(operand, pltpu.HBM)
        for operand in (
            pool,
            sample_index[None, :],
            targets.reshape(2, half, outputs),
            centres,
            coeffs,
            eigvecs,
            eigscale[None, :],
        )
    ])


def solution(mesh):
    return jax.shard_map(
        on_device,
        mesh=mesh,
        in_specs=(
            P("batch", "centre"),
            P("batch"),
            P("batch", None),
            P(("batch", "centre"), None),
            P(("batch", "centre"), None),
            P(("batch", "centre"), None),
            P(),
        ),
        out_specs=P(("batch", "centre"), None),
        check_vma=False,
    )
```

```python
import jax
import jax.numpy as jnp
from jax import lax
from jax.experimental import pallas as pl
from jax.experimental.pallas import tpu as pltpu
from jax.sharding import PartitionSpec as P

MESH = pl.DeviceIdType.MESH
F32 = jnp.float32
BF16 = jnp.bfloat16


def mm(a, b, dims):
    return lax.dot_general(
        a, b, (dims, ((), ())), precision=lax.Precision.HIGHEST, preferred_element_type=F32
    )


def split(value):
    high = value.astype(BF16)
    return high, (value - high.astype(F32)).astype(BF16)


def mm3(a, b, dims):
    def one(left, right):
        return lax.dot_general(left, right, (dims, ((), ())), preferred_element_type=F32)

    rows = a[0].shape[0]
    both = one(jnp.concatenate(a, axis=0), b[0])
    return both[:rows] + (both[rows:] + one(a[0], b[1]))


NN = ((1,), (0,))
NT = ((1,), (1,))


def farthest_first(z, n):
    side = z // (n // 2)
    near = z + side * (n - 1 - 2 * z)
    lone = n - 1 - 2 * near
    order = []
    for k in range(n - 1):
        paired = (k - lone + n) // n
        step = paired * (k - lone)
        beyond = near + (1 - 2 * (step % 2)) * (near - step // 2)
        chip = (1 - paired) * (n - 1 - k) + paired * beyond
        order.append(chip + side * (n - 1 - 2 * chip))
    return order


def flipped(b, k):
    bit = 1
    while bit <= k:
        if k & bit:
            b = b + bit * (1 - 2 * ((b // bit) % 2))
        bit *= 2
    return b


def flat(value):
    count, depth, width = value.shape
    if depth % 8 == 0:
        return value.reshape(count * depth, width)
    return jnp.concatenate([value[j] for j in range(count)], axis=0)


def step_kernel(
    nb, nc, inv_width, model_norm, step_size,
    pool_hbm, i_hbm, t_hbm, z_hbm, a_hbm, e_hbm, s_hbm, out_ref,
    pool_ref, i_ref, t_ref, s_ref, local,
    xg, xs, zp, zh, zl, ep, eq, ej, ca, ks, me, mo, mt, po, fin,
    x_send, x_recv, zp_send, zp_recv, ep_send, ep_recv, eq_send, eq_recv, ej_send, ej_recv,
    cz_send, cz_recv, cp_send, cp_recv, k_send, k_recv, m_send, m_recv, f_send, f_recv,
):
    b = lax.axis_index("batch")
    c = lax.axis_index("centre")
    nz = nc // 2
    nq = 2 * nb
    z = c // 2
    core = lax.rem(c, 2)
    mate = c + 1 - 2 * core
    own = z_hbm.shape[0]
    width = pool_hbm.shape[1]
    half = t_hbm.shape[1]
    plane = nq * own
    q = 2 * b + core
    chips = farthest_first(z, nz)
    rank, parity = z // 2, lax.rem(z, 2)
    sib = z + 1 - 2 * parity
    kin = farthest_first(rank, nz // 2)
    if nb & (nb - 1):
        groups = [lax.rem(b + k, nb) for k in range(1, nb)]
    else:
        groups = [flipped(b, k) for k in range(nb - 1, 0, -1)]
    pending = []

    def push(src, dst, send, recv, bi, ci):
        copy = pltpu.make_async_remote_copy(
            src_ref=src, dst_ref=dst, send_sem=send, recv_sem=recv,
            device_id=(bi, ci), device_id_type=MESH,
        )
        copy.start()
        pending.append(copy)

    def arrived(dst, recv):
        pltpu.make_async_remote_copy(
            src_ref=dst, dst_ref=dst, send_sem=recv, recv_sem=recv,
            device_id=(b, mate), device_id_type=MESH,
        ).wait_recv()

    barrier = pltpu.get_barrier_semaphore()
    for chip in chips:
        for side in (core, 1 - core):
            pl.semaphore_signal(barrier, inc=1, device_id=(b, 2 * chip + side), device_id_type=MESH)
    for bi in groups:
        for ci in (c, mate, 2 * sib, 2 * sib + 1):
            pl.semaphore_signal(barrier, inc=1, device_id=(bi, ci), device_id_type=MESH)
    pl.semaphore_signal(barrier, inc=1, device_id=(b, mate), device_id_type=MESH)
    fetches = []
    for k, (src, dst) in enumerate([
        (pool_hbm, pool_ref), (i_hbm, i_ref), (z_hbm, zp.at[q]), (e_hbm, ep.at[q]),
        (a_hbm, ca.at[z, q]), (s_hbm, s_ref), (t_hbm.at[core], t_ref),
    ]):
        copy = pltpu.make_async_copy(src, dst, local.at[k])
        copy.start()
        fetches.append(copy)
    fetches[0].wait()
    fetches[1].wait()
    rows = i_ref.shape[1]
    lines = lax.broadcasted_iota(jnp.int32, (pool_ref.shape[0], rows), 0)
    chosen = jnp.where(lines == i_ref[...], 1.0, 0.0).astype(F32)
    picked = mm(chosen, pool_ref[...], ((0,), (0,)))
    for h in range(2):
        xg[h] = picked[h * half:(h + 1) * half]
    xs[c] = xg[core]
    for copy in fetches[2:]:
        copy.wait()
    pl.semaphore_wait(barrier, nc - 1 + 4 * (nb - 1))

    for k, chip in enumerate(chips):
        push(ca.at[z, q], ca.at[z, q], cz_send.at[k], cz_recv.at[z], b, 2 * chip + core)
    push(ep.at[q], eq.at[q], eq_send.at[nq], eq_recv.at[q], b, 2 * sib + core)
    for k, chip in enumerate(chips):
        for j, side in enumerate((core, 1 - core)):
            push(xg.at[side], xs.at[c], x_send.at[2 * k + j], x_recv.at[c], b, 2 * chip + side)
    push(xg.at[1 - core], xs.at[c], x_send.at[nc - 2], x_recv.at[c], b, mate)
    for k, other in enumerate(kin):
        push(ep.at[q], ej.at[rank], ej_send.at[k], ej_recv.at[rank], b, 2 * (2 * other + parity) + core)
    for k, bi in enumerate(groups):
        push(zp.at[q], zp.at[q], zp_send.at[k], zp_recv.at[q], bi, c)
    push(zp.at[q], zp.at[q], zp_send.at[nb - 1], zp_recv.at[q], b, mate)
    for k, bi in enumerate(groups):
        push(ep.at[q], ep.at[q], ep_send.at[k], ep_recv.at[q], bi, c)
    push(ep.at[q], ep.at[q], ep_send.at[nb - 1], ep_recv.at[q], b, mate)

    twin = 2 * b + 1 - core
    near = [2 * bi + core for bi in groups]
    cross = [2 * bi + 1 - core for bi in groups]
    arrived(eq.at[q], eq_recv.at[q])
    for k, bi in list(enumerate(groups))[1:]:
        push(eq.at[q], eq.at[q], eq_send.at[k], eq_recv.at[q], bi, c)
    push(eq.at[q], eq.at[q], eq_send.at[nb - 1], eq_recv.at[q], b, mate)
    for chip in chips:
        arrived(ca.at[chip, q], cz_recv.at[chip])
    for k, bi in enumerate(groups):
        push(ca.at[:, q], ca.at[:, q], cp_send.at[k], cp_recv.at[q], bi, c)
    push(ca.at[:, q], ca.at[:, q], cp_send.at[nb - 1], cp_recv.at[q], b, mate)
    for k, qi in enumerate(near):
        arrived(zp.at[qi], zp_recv.at[qi])
        push(zp.at[qi], zp.at[qi], zp_send.at[nb + k], zp_recv.at[qi], b, mate)
    for qi in [twin] + cross:
        arrived(zp.at[qi], zp_recv.at[qi])
    for j in range(nc):
        zh[j], zl[j] = split(flat(zp[:, :, j * width:(j + 1) * width]))

    def score(ci):
        return mm3(split(xs[ci]), (zh[ci], zl[ci]), NT)

    scores = score(c)
    arrived(xs.at[mate], x_recv.at[mate])
    scores = scores + score(mate)
    for k, qi in enumerate(near):
        arrived(ep.at[qi], ep_recv.at[qi])
        push(ep.at[qi], ep.at[qi], ep_send.at[nb + k], ep_recv.at[qi], b, mate)
        if k == 0:
            push(ep.at[qi], eq.at[qi], eq_send.at[0], eq_recv.at[qi], b, 2 * sib + core)
    for chip in chips:
        for side in (core, 1 - core):
            ci = 2 * chip + side
            arrived(xs.at[ci], x_recv.at[ci])
            scores = scores + score(ci)
    kernel = jnp.exp(scores * inv_width)
    ks[z] = kernel
    for k, chip in enumerate(chips):
        push(ks.at[z], ks.at[z], k_send.at[k], k_recv.at[z], b, 2 * chip + core)

    for qi in [twin] + cross:
        arrived(ep.at[qi], ep_recv.at[qi])
    planes = split(flat(ep[...]) * s_ref[...])
    me[parity] = mm3(split(ep[q]), planes, NT)
    me[1 - parity] = mm3(split(eq[q]), planes, NT)
    for k, bi in enumerate(groups):
        push(me, mt.at[rank, :, q], m_send.at[0, k], m_recv.at[rank, parity, q], bi, c)
    push(me, mt.at[rank, :, q], m_send.at[0, nb - 1], m_recv.at[rank, parity, q], b, mate)
    mt[rank, :, q] = me[...]
    for k, qi in enumerate(near):
        arrived(eq.at[qi], eq_recv.at[qi])
        push(eq.at[qi], eq.at[qi], eq_send.at[nb + k], eq_recv.at[qi], b, mate)
    for n, other in enumerate(kin):
        arrived(ej.at[other], ej_recv.at[other])
        lines = split(ej[other])
        here = mt.at[other, parity, q]
        mo[n, 0] = mm3(lines, planes, NT)
        for k, bi in enumerate(groups):
            for j, ci in enumerate((c, mate)):
                push(mo.at[n, 0], here, m_send.at[n + 1, 2 * k + j], m_recv.at[other, parity, q], bi, ci)
        push(mo.at[n, 0], here, m_send.at[n + 1, nq - 2], m_recv.at[other, parity, q], b, mate)
        mt[other, parity, q] = mo[n, 0]
    for qi in [twin] + cross:
        arrived(eq.at[qi], eq_recv.at[qi])
    sibs = split(flat(eq[...]) * s_ref[...])
    for n, other in enumerate(kin):
        lines = split(ej[other])
        here = mt.at[other, parity, q]
        mo[n, 1] = mm3(lines, sibs, NT)
        for k, bi in enumerate(groups):
            for side in range(2):
                push(mo.at[n, 1], here, m_send.at[n + 1, nq + 2 * k + side], m_recv.at[other, parity, q], bi, 2 * sib + side)
        for side in range(2):
            push(mo.at[n, 1], here, m_send.at[n + 1, 2 * nq - 2 + side], m_recv.at[other, parity, q], b, 2 * sib + side)

    for k, qi in enumerate(near):
        arrived(ca.at[:, qi], cp_recv.at[qi])
        push(ca.at[:, qi], ca.at[:, qi], cp_send.at[nb + k], cp_recv.at[qi], b, mate)
    for qi in [twin] + cross:
        arrived(ca.at[:, qi], cp_recv.at[qi])
    for k, qi in enumerate(near):
        arrived(mt.at[rank, :, qi], m_recv.at[rank, parity, qi])
        push(mt.at[rank, :, qi], mt.at[rank, :, qi], m_send.at[0, nb + k], m_recv.at[rank, parity, qi], b, mate)
    value = mm3(split(kernel), split(flat(ca[z])), NN)
    for chip in chips:
        coeffs = split(flat(ca[chip]))
        arrived(ks.at[chip], k_recv.at[chip])
        value = value + mm3(split(ks[chip]), coeffs, NN)
    residual = split(value * model_norm - t_ref[...])

    weights = kernel
    for qi in [twin] + cross:
        arrived(mt.at[rank, :, qi], m_recv.at[rank, parity, qi])
    for n, other in enumerate([rank] + kin):
        if n:
            for qi in [twin] + near + cross:
                arrived(mt.at[other, parity, qi], m_recv.at[other, parity, qi])
            for qi in [q, twin] + near + cross:
                arrived(mt.at[other, 1 - parity, qi], m_recv.at[other, 1 - parity, qi])
        for side in range(2):
            weights = weights - mm3(split(ks[2 * other + side]), split(flat(mt[other, side])), NN)
    partial = mm3(split(weights.T), residual, NN)
    last = nq - 1
    for j in range(nq):
        po[j] = partial[j * own:(j + 1) * own]
    for k, bi in enumerate(groups):
        for j, side in enumerate((core, 1 - core)):
            push(po.at[2 * bi + side], fin.at[q], f_send.at[2 * k + j], f_recv.at[q], bi, 2 * z + side)
    push(po.at[twin], fin.at[q], f_send.at[2 * nb - 2], f_recv.at[q], b, mate)
    total = po[q]
    for copy in pending[:-last]:
        copy.wait_send()
    for qi in [twin] + near + cross:
        arrived(fin.at[qi], f_recv.at[qi])
        total = total + fin[qi]
    out_ref[...] = ca[z, q] - (step_size * model_norm) * total
    for copy in pending[-last:]:
        copy.wait_send()


def on_device(pool, sample_index, targets, centres, coeffs, eigvecs, eigscale):
    nb = lax.axis_size("batch")
    nc = lax.axis_size("centre")
    nz = nc // 2
    nq = 2 * nb
    rows = sample_index.shape[0]
    half = rows // 2
    width = pool.shape[1]
    own, features = centres.shape
    outputs = targets.shape[1]
    eigen = eigvecs.shape[1]
    plane = own * nq
    total_centres = own * nb * nc
    body = lambda *refs: step_kernel(
        nb, nc, features ** -0.5, total_centres ** -0.5,
        0.5 * (total_centres / (rows * nb)) ** 0.5, *refs
    )
    dma = pltpu.SemaphoreType.DMA
    vmem = lambda *dims: pltpu.VMEM(dims, F32)
    scratch = [
        vmem(*pool.shape),
        pltpu.VMEM((1, rows), jnp.int32),
        vmem(half, outputs),
        vmem(1, eigen),
        dma((8,)),
        vmem(2, half, width),
        vmem(nc, half, width),
        vmem(nq, own, features),
        pltpu.VMEM((nc, plane, width), BF16),
        pltpu.VMEM((nc, plane, width), BF16),
        vmem(nq, own, eigen),
        vmem(nq, own, eigen),
        vmem(nz // 2, own, eigen),
        vmem(nz, nq, own, outputs),
        vmem(nz, half, plane),
        vmem(2, own, plane),
        vmem(nz // 2 - 1, 2, own, plane),
        vmem(nz // 2, 2, nq, own, plane),
        vmem(nq, own, outputs),
        vmem(nq, own, outputs),
        dma((nc,)), dma((nc,)),
        dma((nq,)), dma((nq,)),
        dma((nq,)), dma((nq,)),
        dma((nq + 1,)), dma((nq,)),
        dma((nz,)), dma((nz,)),
        dma((nz,)), dma((nz,)),
        dma((nq,)), dma((nq,)),
        dma((nz,)), dma((nz,)),
        dma((nz // 2, 2 * nq)), dma((nz // 2, 2, nq)),
        dma((nq,)), dma((nq,)),
    ]
    taken = 0
    for buffer in scratch:
        if buffer.memory_space == pltpu.VMEM:
            *outer, deep, wide = buffer.shape
            size = -(-deep // 8) * 8 * (-(-wide // 128) * 128) * 4
            for extent in outer:
                size *= extent
            taken += size
    return pl.pallas_call(
        body,
        out_shape=jax.ShapeDtypeStruct((own, outputs), F32),
        in_specs=[pl.BlockSpec(memory_space=pltpu.HBM)] * 7,
        out_specs=pl.BlockSpec(memory_space=pltpu.VMEM),
        scratch_shapes=scratch,
        compiler_params=pltpu.CompilerParams(
            collective_id=0, has_side_effects=True, vmem_limit_bytes=min(taken + (12 << 20), 67043328)
        ),
    )(*[
        pltpu.with_memory_space_constraint(operand, pltpu.HBM)
        for operand in (
            pool,
            sample_index[None, :],
            targets.reshape(2, half, outputs),
            centres,
            coeffs,
            eigvecs,
            eigscale[None, :],
        )
    ])


def solution(mesh):
    return jax.shard_map(
        on_device,
        mesh=mesh,
        in_specs=(
            P("batch", "centre"),
            P("batch"),
            P("batch", None),
            P(("batch", "centre"), None),
            P(("batch", "centre"), None),
            P(("batch", "centre"), None),
            P(),
        ),
        out_specs=P(("batch", "centre"), None),
        check_vma=False,
    )
```

```python
import jax
import jax.numpy as jnp
from jax import lax
from jax.experimental import pallas as pl
from jax.experimental.pallas import tpu as pltpu
from jax.sharding import PartitionSpec as P

MESH = pl.DeviceIdType.MESH
F32 = jnp.float32
BF16 = jnp.bfloat16


def mm(a, b, dims):
    return lax.dot_general(
        a, b, (dims, ((), ())), precision=lax.Precision.HIGHEST, preferred_element_type=F32
    )


def split(value):
    high = value.astype(BF16)
    return high, (value - high.astype(F32)).astype(BF16)


def mm3(a, b, dims):
    def one(left, right):
        return lax.dot_general(left, right, (dims, ((), ())), preferred_element_type=F32)

    rows = a[0].shape[0]
    both = one(jnp.concatenate(a, axis=0), b[0])
    return both[:rows] + (both[rows:] + one(a[0], b[1]))


NN = ((1,), (0,))
NT = ((1,), (1,))


def farthest_first(z, n):
    side = z // (n // 2)
    near = z + side * (n - 1 - 2 * z)
    lone = n - 1 - 2 * near
    order = []
    for k in range(n - 1):
        paired = (k - lone + n) // n
        step = paired * (k - lone)
        beyond = near + (1 - 2 * (step % 2)) * (near - step // 2)
        chip = (1 - paired) * (n - 1 - k) + paired * beyond
        order.append(chip + side * (n - 1 - 2 * chip))
    return order


def flipped(b, k):
    bit = 1
    while bit <= k:
        if k & bit:
            b = b + bit * (1 - 2 * ((b // bit) % 2))
        bit *= 2
    return b


def flat(value):
    count, depth, width = value.shape
    if depth % 8 == 0:
        return value.reshape(count * depth, width)
    return jnp.concatenate([value[j] for j in range(count)], axis=0)


def step_kernel(
    nb, nc, inv_width, model_norm, step_size,
    pool_hbm, i_hbm, t_hbm, z_hbm, a_hbm, e_hbm, s_hbm, out_ref,
    pool_ref, i_ref, t_ref, s_ref, local,
    xg, xs, zp, zh, zl, ep, eq, ej, ca, ks, gh, gl, me, mo, mt, po, fin,
    x_send, x_recv, zp_send, zp_recv, ep_send, ep_recv, eq_send, eq_recv, ej_send, ej_recv,
    cz_send, cz_recv, cp_send, cp_recv, k_send, k_recv, m_send, m_recv, f_send, f_recv,
):
    b = lax.axis_index("batch")
    c = lax.axis_index("centre")
    nz = nc // 2
    nq = 2 * nb
    z = c // 2
    core = lax.rem(c, 2)
    mate = c + 1 - 2 * core
    own = z_hbm.shape[0]
    width = pool_hbm.shape[1]
    half = t_hbm.shape[1]
    plane = nq * own
    q = 2 * b + core
    chips = farthest_first(z, nz)
    rank, parity = z // 2, lax.rem(z, 2)
    sib = z + 1 - 2 * parity
    kin = farthest_first(rank, nz // 2)
    if nb & (nb - 1):
        groups = [lax.rem(b + k, nb) for k in range(1, nb)]
    else:
        groups = [flipped(b, k) for k in range(nb - 1, 0, -1)]
    pending = []

    def push(src, dst, send, recv, bi, ci):
        copy = pltpu.make_async_remote_copy(
            src_ref=src, dst_ref=dst, send_sem=send, recv_sem=recv,
            device_id=(bi, ci), device_id_type=MESH,
        )
        copy.start()
        pending.append(copy)

    def arrived(dst, recv):
        pltpu.make_async_remote_copy(
            src_ref=dst, dst_ref=dst, send_sem=recv, recv_sem=recv,
            device_id=(b, mate), device_id_type=MESH,
        ).wait_recv()

    barrier = pltpu.get_barrier_semaphore()
    for chip in chips:
        for side in (core, 1 - core):
            pl.semaphore_signal(barrier, inc=1, device_id=(b, 2 * chip + side), device_id_type=MESH)
    for bi in groups:
        for ci in (c, mate, 2 * sib, 2 * sib + 1):
            pl.semaphore_signal(barrier, inc=1, device_id=(bi, ci), device_id_type=MESH)
    pl.semaphore_signal(barrier, inc=1, device_id=(b, mate), device_id_type=MESH)
    fetches = []
    for k, (src, dst) in enumerate([
        (pool_hbm, pool_ref), (i_hbm, i_ref), (z_hbm, zp.at[q]), (e_hbm, ep.at[q]),
        (a_hbm, ca.at[z, q]), (s_hbm, s_ref), (t_hbm.at[core], t_ref),
    ]):
        copy = pltpu.make_async_copy(src, dst, local.at[k])
        copy.start()
        fetches.append(copy)
    fetches[0].wait()
    fetches[1].wait()
    rows = i_ref.shape[1]
    lines = lax.broadcasted_iota(jnp.int32, (pool_ref.shape[0], rows), 0)
    chosen = jnp.where(lines == i_ref[...], 1.0, 0.0).astype(F32)
    picked = mm(chosen, pool_ref[...], ((0,), (0,)))
    for h in range(2):
        xg[h] = picked[h * half:(h + 1) * half]
    xs[c] = xg[core]
    for copy in fetches[2:]:
        copy.wait()
    pl.semaphore_wait(barrier, nc - 1 + 4 * (nb - 1))

    for k, chip in enumerate(chips):
        push(ca.at[z, q], ca.at[z, q], cz_send.at[k], cz_recv.at[z], b, 2 * chip + core)
    push(ep.at[q], eq.at[q], eq_send.at[nq], eq_recv.at[q], b, 2 * sib + core)
    for k, chip in enumerate(chips):
        for j, side in enumerate((core, 1 - core)):
            push(xg.at[side], xs.at[c], x_send.at[2 * k + j], x_recv.at[c], b, 2 * chip + side)
    push(xg.at[1 - core], xs.at[c], x_send.at[nc - 2], x_recv.at[c], b, mate)
    for k, other in enumerate(kin):
        push(ep.at[q], ej.at[rank], ej_send.at[k], ej_recv.at[rank], b, 2 * (2 * other + parity) + core)
    for k, bi in enumerate(groups):
        push(zp.at[q], zp.at[q], zp_send.at[k], zp_recv.at[q], bi, c)
    push(zp.at[q], zp.at[q], zp_send.at[nb - 1], zp_recv.at[q], b, mate)
    for k, bi in enumerate(groups):
        push(ep.at[q], ep.at[q], ep_send.at[k], ep_recv.at[q], bi, c)
    push(ep.at[q], ep.at[q], ep_send.at[nb - 1], ep_recv.at[q], b, mate)

    twin = 2 * b + 1 - core
    near = [2 * bi + core for bi in groups]
    cross = [2 * bi + 1 - core for bi in groups]
    arrived(eq.at[q], eq_recv.at[q])
    for k, bi in list(enumerate(groups))[1:]:
        push(eq.at[q], eq.at[q], eq_send.at[k], eq_recv.at[q], bi, c)
    push(eq.at[q], eq.at[q], eq_send.at[nb - 1], eq_recv.at[q], b, mate)
    for chip in chips:
        arrived(ca.at[chip, q], cz_recv.at[chip])
    for k, bi in enumerate(groups):
        push(ca.at[:, q], ca.at[:, q], cp_send.at[k], cp_recv.at[q], bi, c)
    push(ca.at[:, q], ca.at[:, q], cp_send.at[nb - 1], cp_recv.at[q], b, mate)
    for k, qi in enumerate(near):
        arrived(zp.at[qi], zp_recv.at[qi])
        push(zp.at[qi], zp.at[qi], zp_send.at[nb + k], zp_recv.at[qi], b, mate)
    for qi in [twin] + cross:
        arrived(zp.at[qi], zp_recv.at[qi])
    for j in range(nc):
        zh[j], zl[j] = split(flat(zp[:, :, j * width:(j + 1) * width]))

    def score(ci):
        return mm3(split(xs[ci]), (zh[ci], zl[ci]), NT)

    scores = score(c)
    arrived(xs.at[mate], x_recv.at[mate])
    scores = scores + score(mate)
    for k, qi in enumerate(near):
        arrived(ep.at[qi], ep_recv.at[qi])
        push(ep.at[qi], ep.at[qi], ep_send.at[nb + k], ep_recv.at[qi], b, mate)
        if k == 0:
            push(ep.at[qi], eq.at[qi], eq_send.at[0], eq_recv.at[qi], b, 2 * sib + core)
    for chip in chips:
        for side in (core, 1 - core):
            ci = 2 * chip + side
            arrived(xs.at[ci], x_recv.at[ci])
            scores = scores + score(ci)
    kernel = jnp.exp(scores * inv_width)
    ks[z] = kernel
    for k, chip in enumerate(chips):
        push(ks.at[z], ks.at[z], k_send.at[k], k_recv.at[z], b, 2 * chip + core)

    for qi in [twin] + cross:
        arrived(ep.at[qi], ep_recv.at[qi])
    planes = split(flat(ep[...]) * s_ref[...])
    me[parity] = mm3(split(ep[q]), planes, NT)
    me[1 - parity] = mm3(split(eq[q]), planes, NT)
    for k, bi in enumerate(groups):
        push(me, mt.at[rank, :, q], m_send.at[0, k], m_recv.at[rank, parity, q], bi, c)
    push(me, mt.at[rank, :, q], m_send.at[0, nb - 1], m_recv.at[rank, parity, q], b, mate)
    mt[rank, :, q] = me[...]
    for k, qi in enumerate(near):
        arrived(eq.at[qi], eq_recv.at[qi])
        push(eq.at[qi], eq.at[qi], eq_send.at[nb + k], eq_recv.at[qi], b, mate)
    for n, other in enumerate(kin):
        arrived(ej.at[other], ej_recv.at[other])
        lines = split(ej[other])
        here = mt.at[other, parity, q]
        mo[n, 0] = mm3(lines, planes, NT)
        for k, bi in enumerate(groups):
            for j, ci in enumerate((c, mate)):
                push(mo.at[n, 0], here, m_send.at[n + 1, 2 * k + j], m_recv.at[other, parity, q], bi, ci)
        push(mo.at[n, 0], here, m_send.at[n + 1, nq - 2], m_recv.at[other, parity, q], b, mate)
        mt[other, parity, q] = mo[n, 0]
    for qi in [twin] + cross:
        arrived(eq.at[qi], eq_recv.at[qi])
    sibs = split(flat(eq[...]) * s_ref[...])
    for n, other in enumerate(kin):
        lines = split(ej[other])
        here = mt.at[other, parity, q]
        mo[n, 1] = mm3(lines, sibs, NT)
        for k, bi in enumerate(groups):
            for side in range(2):
                push(mo.at[n, 1], here, m_send.at[n + 1, nq + 2 * k + side], m_recv.at[other, parity, q], bi, 2 * sib + side)
        for side in range(2):
            push(mo.at[n, 1], here, m_send.at[n + 1, 2 * nq - 2 + side], m_recv.at[other, parity, q], b, 2 * sib + side)

    for k, qi in enumerate(near):
        arrived(ca.at[:, qi], cp_recv.at[qi])
        push(ca.at[:, qi], ca.at[:, qi], cp_send.at[nb + k], cp_recv.at[qi], b, mate)
    for qi in [twin] + cross:
        arrived(ca.at[:, qi], cp_recv.at[qi])
    for k, qi in enumerate(near):
        arrived(mt.at[rank, :, qi], m_recv.at[rank, parity, qi])
        push(mt.at[rank, :, qi], mt.at[rank, :, qi], m_send.at[0, nb + k], m_recv.at[rank, parity, qi], b, mate)
    value = mm3(split(kernel), split(flat(ca[z])), NN)
    for chip in chips:
        coeffs = split(flat(ca[chip]))
        arrived(ks.at[chip], k_recv.at[chip])
        value = value + mm3(split(ks[chip]), coeffs, NN)
    residual = split(value * model_norm - t_ref[...])

    for j in range(nz):
        gh[j], gl[j] = split(mm3(split(ks[j].T), residual, NN))
    partial = mm3(split(kernel.T), residual, NN)
    for qi in [twin] + cross:
        arrived(mt.at[rank, :, qi], m_recv.at[rank, parity, qi])
    for n, other in enumerate([rank] + kin):
        if n:
            for qi in [twin] + near + cross:
                arrived(mt.at[other, parity, qi], m_recv.at[other, parity, qi])
            for qi in [q, twin] + near + cross:
                arrived(mt.at[other, 1 - parity, qi], m_recv.at[other, 1 - parity, qi])
        for side in range(2):
            field = (gh[2 * other + side], gl[2 * other + side])
            partial = partial - mm3(split(flat(mt[other, side]).T), field, NN)
    last = nq - 1
    for j in range(nq):
        po[j] = partial[j * own:(j + 1) * own]
    for k, bi in enumerate(groups):
        for j, side in enumerate((core, 1 - core)):
            push(po.at[2 * bi + side], fin.at[q], f_send.at[2 * k + j], f_recv.at[q], bi, 2 * z + side)
    push(po.at[twin], fin.at[q], f_send.at[2 * nb - 2], f_recv.at[q], b, mate)
    total = po[q]
    for copy in pending[:-last]:
        copy.wait_send()
    for qi in [twin] + near + cross:
        arrived(fin.at[qi], f_recv.at[qi])
        total = total + fin[qi]
    out_ref[...] = ca[z, q] - (step_size * model_norm) * total
    for copy in pending[-last:]:
        copy.wait_send()


def on_device(pool, sample_index, targets, centres, coeffs, eigvecs, eigscale):
    nb = lax.axis_size("batch")
    nc = lax.axis_size("centre")
    nz = nc // 2
    nq = 2 * nb
    rows = sample_index.shape[0]
    half = rows // 2
    width = pool.shape[1]
    own, features = centres.shape
    outputs = targets.shape[1]
    eigen = eigvecs.shape[1]
    plane = own * nq
    total_centres = own * nb * nc
    body = lambda *refs: step_kernel(
        nb, nc, features ** -0.5, total_centres ** -0.5,
        0.5 * (total_centres / (rows * nb)) ** 0.5, *refs
    )
    dma = pltpu.SemaphoreType.DMA
    vmem = lambda *dims: pltpu.VMEM(dims, F32)
    scratch = [
        vmem(*pool.shape),
        pltpu.VMEM((1, rows), jnp.int32),
        vmem(half, outputs),
        vmem(1, eigen),
        dma((8,)),
        vmem(2, half, width),
        vmem(nc, half, width),
        vmem(nq, own, features),
        pltpu.VMEM((nc, plane, width), BF16),
        pltpu.VMEM((nc, plane, width), BF16),
        vmem(nq, own, eigen),
        vmem(nq, own, eigen),
        vmem(nz // 2, own, eigen),
        vmem(nz, nq, own, outputs),
        vmem(nz, half, plane),
        pltpu.VMEM((nz, plane, outputs), BF16),
        pltpu.VMEM((nz, plane, outputs), BF16),
        vmem(2, own, plane),
        vmem(nz // 2 - 1, 2, own, plane),
        vmem(nz // 2, 2, nq, own, plane),
        vmem(nq, own, outputs),
        vmem(nq, own, outputs),
        dma((nc,)), dma((nc,)),
        dma((nq,)), dma((nq,)),
        dma((nq,)), dma((nq,)),
        dma((nq + 1,)), dma((nq,)),
        dma((nz,)), dma((nz,)),
        dma((nz,)), dma((nz,)),
        dma((nq,)), dma((nq,)),
        dma((nz,)), dma((nz,)),
        dma((nz // 2, 2 * nq)), dma((nz // 2, 2, nq)),
        dma((nq,)), dma((nq,)),
    ]
    taken = 0
    for buffer in scratch:
        if buffer.memory_space == pltpu.VMEM:
            *outer, deep, wide = buffer.shape
            size = -(-deep // 8) * 8 * (-(-wide // 128) * 128) * 4
            for extent in outer:
                size *= extent
            taken += size
    return pl.pallas_call(
        body,
        out_shape=jax.ShapeDtypeStruct((own, outputs), F32),
        in_specs=[pl.BlockSpec(memory_space=pltpu.HBM)] * 7,
        out_specs=pl.BlockSpec(memory_space=pltpu.VMEM),
        scratch_shapes=scratch,
        compiler_params=pltpu.CompilerParams(
            collective_id=0, has_side_effects=True, vmem_limit_bytes=min(taken + (12 << 20), 67043328)
        ),
    )(*[
        pltpu.with_memory_space_constraint(operand, pltpu.HBM)
        for operand in (
            pool,
            sample_index[None, :],
            targets.reshape(2, half, outputs),
            centres,
            coeffs,
            eigvecs,
            eigscale[None, :],
        )
    ])


def solution(mesh):
    return jax.shard_map(
        on_device,
        mesh=mesh,
        in_specs=(
            P("batch", "centre"),
            P("batch"),
            P("batch", None),
            P(("batch", "centre"), None),
            P(("batch", "centre"), None),
            P(("batch", "centre"), None),
            P(),
        ),
        out_specs=P(("batch", "centre"), None),
        check_vma=False,
    )
```
